32 devices in a mesh: row: 4 (over y, x), col: 8 (over z, core).
Axes of the slice: x: 2, y: 2, z: 4, core: 2. Of those that a mesh axis runs over, the one named last changes fastest.
Arguments:
- pair_states: bfloat16 [1024, 16384], P(None, ('row', 'col')), may hold values from -0.046875 to 0.046875
- screening: bfloat16 [4, 16384, 16384], P(None, 'row', 'col'), may hold values from -6 to 6
- qp_energy: float32 [8], replicated, may hold values from -0.5 to 0.5
- band_energy: float32 [2048], replicated, may hold values from -2 to 2
- band_index: int32 [128], replicated, may hold values from 0 to 2047
- nodes: float32 [4], replicated, may hold values from 0.1 to 2
- node_weights: float32 [4], replicated, may hold values from 0.05 to 1
Outputs:
- contrib: float32 [8, 128], replicated
- sigma: float32 [8], replicated
The draws below stay inside these ranges and needn't reach their ends.
All inputs are finite; a program needn't handle non-finite values.
Results may differ from the reference program's by a relative error of at most 0.0003.
Values may be sent and summed in bfloat16 or wider, within the bound.
A program may use at most 128 MiB of HBM per device.

```python
import math
import jax
import jax.numpy as jnp
from jax import lax

NG = 16384
FREQS = 4
NQ = 8
NM = 128
NBANDS = 2048
PAIRS = 1024


def plant(result, rng, least, top_value):
    dims = result.shape
    place = [jax.random.randint(jax.random.fold_in(rng, axis), (), 0, dims[axis]) for axis in range(len(dims))]
    result = result.at[tuple(place)].set(least)
    longest = dims.index(max(dims))
    place[longest] = (place[longest] + 1) % dims[longest]
    return result.at[tuple(place)].set(top_value)


def levels(rng, extent, cuts, least, largest):
    gain, own = 1.0, jax.random.fold_in(rng, 6)
    for axis_at, shards_of in cuts:
        heights = jnp.exp(jax.random.uniform(jax.random.fold_in(own, axis_at), (shards_of,), jnp.float32, least / len(cuts), largest / len(cuts)))
        gain = gain * jnp.repeat(heights, extent[axis_at] // shards_of).reshape([-1 if axis == axis_at else 1 for axis in range(len(extent))])
    return gain


def noise(rng, dims, width, reach, pieces=(), held_as=jnp.bfloat16):
    values = jax.random.normal(rng, dims, jnp.float32) * width
    if len(pieces) > 0:
        values = levels(rng, dims, pieces, -0.22, 0.18) * values
    return jnp.clip(values, min=-reach, max=reach).astype(held_as)


def setup_inputs(seed: int = 0) -> dict:
    key_of = jax.random.split(jax.random.key(seed), 8)
    return {
        "pair_states": noise(key_of[0], (PAIRS, NG), NG ** -0.5, 0.046875, ((1, 32),)),
        "screening": noise(key_of[1], (FREQS, NG, NG), 1.0, 6.0, ((1, 4), (2, 8))),
        "qp_energy": jnp.clip(jax.random.uniform(key_of[2], (NQ,), jnp.float32, -0.5, 0.5), -0.5, 0.5),
        "band_energy": jnp.clip(jax.random.uniform(key_of[3], (NBANDS,), jnp.float32, -2.0, 2.0), -2.0, 2.0),
        "band_index": plant(jax.random.randint(key_of[4], (NM,), 0, NBANDS), jax.random.fold_in(key_of[4], 1), 0, NBANDS - 1).astype(jnp.int32),
        "nodes": jnp.clip(jnp.exp(jax.random.uniform(key_of[5], (FREQS,), jnp.float32, math.log(0.1), math.log(2.0))), 0.1, 2.0),
        "node_weights": jnp.clip(jnp.exp(jax.random.uniform(key_of[6], (FREQS,), jnp.float32, math.log(0.05), math.log(1.0))), 0.05, 1.0),
    }


def reference(pair_states, screening, qp_energy, band_energy, band_index, nodes, node_weights):
    states = pair_states.astype(jnp.float32)

    def one_node(layer):
        image = jnp.dot(states, layer.astype(jnp.float32), precision=lax.Precision.HIGHEST, preferred_element_type=jnp.float32)
        return jnp.sum(image * states, axis=1)

    quad = lax.map(one_node, screening)
    table = jnp.arange(NBANDS).astype(jnp.int32)
    chosen = jnp.sum(jnp.where(band_index[:, None] == table[None, :], band_energy[None, :], jnp.float32(0.0)), axis=1)
    gap = (qp_energy[:, None] - chosen[None, :]).reshape(-1)
    factor = node_weights[:, None] * gap[None, :] / (gap[None, :] * gap[None, :] + nodes[:, None] * nodes[:, None])
    contrib = jnp.sum(factor * quad, axis=0).reshape(NQ, NM)
    sigma = jnp.sum(contrib, axis=1)
    return contrib, sigma
```

```python
import functools

import jax
import jax.numpy as jnp
from jax import lax
from jax.experimental import pallas as pl
from jax.experimental.pallas import tpu as pltpu
from jax.sharding import PartitionSpec as P

MESH = pl.DeviceIdType.MESH
CORES = 2


def orders(chips):
    table = []
    for here in range(chips):
        steps = [(here, 0), (here, 1)]
        for reach in range(1, chips):
            near = [other for other in (here - reach, here + reach) if 0 <= other < chips]
            steps += [(other, 0) for other in near] + [(other, 1) for other in near]
        table.append(steps)
    return table


def relay_steps(chips):
    return [2 * reach for reach in range(1, chips)]


def pick(table, row, column):
    value = jnp.int32(0)
    for i, line in enumerate(table):
        for j, entry in enumerate(line):
            if entry:
                value = jnp.where((row == i) & (column == j), jnp.int32(entry), value)
    return value


def kernel(
    rows, columns, own_ref, w_ref, factor_ref, out_ref,
    panel, cols, acc, tiles, quad, near_sum, far_sum,
    tile_sem, own_sem, send_sem, recv_sem, col_send, col_recv, near_send, near_recv, far_send, far_recv,
):
    row, column = lax.axis_index("row"), lax.axis_index("col")
    chips = columns // CORES
    chip, core = column // CORES, column % CORES
    partner = column + 1 - 2 * core
    freqs, _, width = w_ref.shape
    depth = own_ref.shape[1]
    pieces = width // depth
    pairs = own_ref.shape[0]
    table = orders(chips)
    steps = columns

    def at(r, c):
        return {"row": r, "col": c}

    barrier = pltpu.get_barrier_semaphore()
    linear = row * columns + column
    to_row, to_col = linear % pieces, linear // pieces
    stays = (to_row == row) & (to_col == column)
    first = row * 0 + column * pieces + row
    from_row, from_col = first // columns, first % columns
    for other in range(1, columns):
        pl.semaphore_signal(barrier, inc=1, device_id=at(row, (column + other) % columns), device_id_type=MESH)
    for other in range(1, rows):
        pl.semaphore_signal(barrier, inc=1, device_id=at((row + other) % rows, column), device_id_type=MESH)

    @pl.when(jnp.logical_not(stays))
    def _():
        pl.semaphore_signal(barrier, inc=1, device_id=at(to_row, to_col), device_id_type=MESH)
        pl.semaphore_signal(barrier, inc=1, device_id=at(from_row, from_col), device_id_type=MESH)

    def slot_of(step):
        source = pick([[s[0] for s in line] for line in table], chip, step)
        other = pick([[s[1] for s in line] for line in table], chip, step)
        return source * CORES + jnp.where(other == 1, 1 - core, core)

    def tile_copy(index):
        step, freq = index // freqs, index % freqs
        lines = pl.ds(pl.multiple_of(slot_of(step) * depth, depth), depth)
        spot = index % tiles.shape[0]
        return pltpu.make_async_copy(w_ref.at[freq, lines, :], tiles.at[spot], tile_sem.at[spot])

    ahead = tiles.shape[0] - 1
    for index in range(ahead):
        tile_copy(index).start()
    own_copy = pltpu.make_async_copy(own_ref, panel.at[column], own_sem)
    own_copy.start()

    pl.semaphore_wait(barrier, columns + rows - 2 + jnp.where(stays, 0, 2))
    own_copy.wait()

    def pass_on(source, way):
        slot = source * CORES + core
        target = [column + CORES, column - CORES, partner][way]
        return pltpu.make_async_remote_copy(
            src_ref=panel.at[slot], dst_ref=panel.at[slot], send_sem=send_sem.at[way, source],
            recv_sem=recv_sem.at[slot], device_id=at(row, target), device_id_type=MESH,
        )

    def goes(source, way):
        if way == 0:
            return (source <= chip) & (chip < chips - 1)
        return (source >= chip) & (chip > 0)

    def forward(source):
        for way in (0, 1):

            @pl.when(goes(source, way))
            def _():
                pass_on(source, way).start()

        pass_on(source, 2).start()

    def arrive(slot):
        pltpu.make_async_copy(panel.at[slot], panel.at[slot], recv_sem.at[slot]).wait()

    def col_first():
        return pltpu.make_async_remote_copy(
            src_ref=panel.at[column], dst_ref=cols.at[to_row], send_sem=col_send.at[0],
            recv_sem=col_recv.at[to_row], device_id=at(to_row, to_col), device_id_type=MESH,
        )

    def col_local():
        return pltpu.make_async_copy(panel.at[column], cols.at[row], col_recv.at[row])

    def col_next(other):
        return pltpu.make_async_remote_copy(
            src_ref=cols.at[row], dst_ref=cols.at[row], send_sem=col_send.at[other],
            recv_sem=col_recv.at[row], device_id=at((row + other) % rows, column), device_id_type=MESH,
        )

    def col_arrive(slot):
        pltpu.make_async_copy(cols.at[slot], cols.at[slot], col_recv.at[slot]).wait()

    forward(chip)

    @pl.when(jnp.logical_not(stays))
    def _():
        col_first().start()

    @pl.when(stays)
    def _():
        col_local().start()

    def product(slot, spot, piece):
        return jnp.dot(
            panel[slot], tiles[spot, :, pl.ds(pl.multiple_of(piece * depth, depth), depth)],
            preferred_element_type=jnp.float32,
        )

    def each(step, work):
        slot = slot_of(step)

        @pl.loop(0, freqs)
        def _(freq):
            index = step * freqs + freq
            spot = index % tiles.shape[0]

            @pl.when(index + ahead < steps * freqs)
            def _():
                tile_copy(index + ahead).start()

            tile_copy(index).wait()

            @pl.loop(0, pieces)
            def _(piece):
                work(freq, piece, product(slot, spot, piece))

    def at_piece(piece):
        return pl.ds(pl.multiple_of(piece * depth, depth), depth)

    def store(freq, piece, value):
        acc[freq, :, at_piece(piece)] = value

    def add(freq, piece, value):
        acc[freq, :, at_piece(piece)] += value

    def close(freq, piece, value):
        total = (acc[freq, :, at_piece(piece)] + value) * cols[piece].astype(jnp.float32)
        part = total[:, :128]
        for lane in range(128, depth, 128):
            part = part + total[:, lane : lane + 128]

        @pl.when(piece == 0)
        def _():
            quad[freq] = part

        @pl.when(piece > 0)
        def _():
            quad[freq] += part

    each(0, store)

    def sides(reach, work):
        for source in (chip - reach, chip + reach):

            @pl.when((source >= 0) & (source < chips))
            def _():
                work(source)

    def prepare(step):
        for reach, when in enumerate(relay_steps(chips), 1):

            @pl.when(step == when)
            def _():
                def one(source):
                    arrive(source * CORES + core)
                    forward(source)

                sides(reach, one)

        @pl.when(step == COL_STEP)
        def _():
            col_arrive(row)
            for other in range(1, rows):
                col_next(other).start()

        slot = slot_of(step)

        @pl.when(slot % CORES != core)
        def _():
            arrive(slot)

    @pl.loop(1, steps - 1)
    def _(step):
        prepare(step)
        each(step, add)

    prepare(steps - 1)
    for other in range(1, rows):
        col_arrive((row + other) % rows)
    each(steps - 1, close)

    bands = pairs // 128
    lines = []
    for band in range(bands):
        line = jnp.zeros((1, 128), jnp.float32)
        for freq in range(freqs):
            turned = quad[freq, pl.ds(band * 128, 128), :].T
            line = line + jnp.sum(turned, axis=0, keepdims=True) * factor_ref[freq, pl.ds(band, 1), :]
        lines.append(line)
    near_sum[column] = jnp.concatenate(lines, axis=0)

    def near(other):
        return pltpu.make_async_remote_copy(
            src_ref=near_sum.at[column], dst_ref=near_sum.at[column], send_sem=near_send.at[other],
            recv_sem=near_recv.at[column], device_id=at(row, (column + other) % columns), device_id_type=MESH,
        )

    def far(other):
        return pltpu.make_async_remote_copy(
            src_ref=far_sum.at[row], dst_ref=far_sum.at[row], send_sem=far_send.at[other],
            recv_sem=far_recv.at[row], device_id=at((row + other) % rows, column), device_id_type=MESH,
        )

    for other in range(1, columns):
        near(other).start()
    for other in range(1, columns):
        slot = (column + other) % columns
        pltpu.make_async_copy(near_sum.at[slot], near_sum.at[slot], near_recv.at[slot]).wait()
    total = near_sum[0]
    for slot in range(1, columns):
        total = total + near_sum[slot]
    far_sum[row] = total
    for other in range(1, rows):
        far(other).start()
    for other in range(1, rows):
        slot = (row + other) % rows
        pltpu.make_async_copy(far_sum.at[slot], far_sum.at[slot], far_recv.at[slot]).wait()
    total = far_sum[0]
    for slot in range(1, rows):
        total = total + far_sum[slot]
    out_ref[...] = total

    def sent(source):
        for way in (0, 1):

            @pl.when(goes(source, way))
            def _():
                pass_on(source, way).wait_send()

        pass_on(source, 2).wait_send()

    for source in range(chips):
        sent(source)

    @pl.when(jnp.logical_not(stays))
    def _():
        col_first().wait_send()

    for other in range(1, rows):
        col_next(other).wait_send()
        far(other).wait_send()
    for other in range(1, columns):
        near(other).wait_send()


def weights(qp_energy, band_energy, band_index, nodes, node_weights):
    table = lax.broadcasted_iota(jnp.int32, (band_index.shape[0], band_energy.shape[0]), 1)
    chosen = jnp.sum(
        jnp.where(band_index[:, None] == table, band_energy[None, :], jnp.float32(0.0)), axis=1
    )
    gap = (qp_energy[:, None] - chosen[None, :])[None]
    return node_weights[:, None, None] * gap / (gap * gap + (nodes * nodes)[:, None, None])


COL_STEP = 3


def fused(pair_states, screening, qp_energy, band_energy, band_index, nodes, node_weights):
    rows, columns = lax.axis_size("row"), lax.axis_size("col")
    pairs, depth = pair_states.shape
    freqs, _, width = screening.shape
    factor = weights(qp_energy, band_energy, band_index, nodes, node_weights)
    shape = (qp_energy.shape[0], band_index.shape[0])
    dma = pltpu.SemaphoreType.DMA
    contrib = pl.pallas_call(
        functools.partial(kernel, rows, columns),
        out_shape=jax.ShapeDtypeStruct(shape, jnp.float32),
        in_specs=[
            pl.BlockSpec(memory_space=pl.ANY),
            pl.BlockSpec(memory_space=pl.ANY),
            pl.BlockSpec(memory_space=pltpu.VMEM),
        ],
        out_specs=pl.BlockSpec(memory_space=pltpu.VMEM),
        scratch_shapes=[
            pltpu.VMEM((columns, pairs, depth), jnp.bfloat16),
            pltpu.VMEM((width // depth, pairs, depth), jnp.bfloat16),
            pltpu.VMEM((freqs, pairs, width), jnp.float32),
            pltpu.VMEM((3, depth, width), jnp.bfloat16),
            pltpu.VMEM((freqs, pairs, 128), jnp.float32),
            pltpu.VMEM((columns,) + shape, jnp.float32),
            pltpu.VMEM((rows,) + shape, jnp.float32),
            dma((3,)),
            dma,
            dma((3, columns // CORES)),
            dma((columns,)),
            dma((rows,)),
            dma((rows,)),
            dma((columns,)),
            dma((columns,)),
            dma((rows,)),
            dma((rows,)),
        ],
        compiler_params=pltpu.CompilerParams(
            collective_id=0, has_side_effects=True, vmem_limit_bytes=67043328
        ),
        cost_estimate=pl.CostEstimate(
            flops=2 * freqs * pairs * columns * depth * width,
            bytes_accessed=freqs * columns * depth * width * 2,
            transcendentals=0,
        ),
    )(pair_states, screening, factor)
    return contrib, jnp.sum(contrib, axis=1)


def broadcast(block, axis, holder):
    block = jnp.where(lax.axis_index(axis) == holder, block, jnp.zeros_like(block))
    return lax.psum(block, axis)


def shards(pair_states, screening, qp_energy, band_energy, band_index, nodes, node_weights):
    width = screening.shape[2]
    panel = lax.all_gather(pair_states, "col", axis=1, tiled=True)
    images = jnp.einsum("pg,fgc->fpc", panel, screening, preferred_element_type=jnp.float32)
    ratio = lax.axis_size("col") // lax.axis_size("row")
    column = lax.axis_index("col")
    offset = column % ratio * width
    own_piece = lax.dynamic_slice_in_dim(panel, offset, width, 1)
    col_states = broadcast(own_piece, "row", column // ratio)
    partial_value = jnp.sum(images * col_states.astype(jnp.float32)[None, :, :], axis=2)
    table = lax.broadcasted_iota(jnp.int32, (band_index.shape[0], band_energy.shape[0]), 1)
    chosen = jnp.sum(
        jnp.where(band_index[:, None] == table, band_energy[None, :], jnp.float32(0.0)), axis=1
    )
    gap = (qp_energy[:, None] - chosen[None, :]).reshape(-1)
    factor = (
        node_weights[:, None]
        * gap[None, :]
        / (gap[None, :] * gap[None, :] + nodes[:, None] * nodes[:, None])
    )
    flat = lax.psum(jnp.sum(factor * partial_value, axis=0), ("row", "col"))
    contrib = flat.reshape(qp_energy.shape[0], band_index.shape[0])
    sigma = jnp.sum(contrib, axis=1)
    return (contrib, sigma)


def step(pair_states, screening, *others):
    rows, columns = lax.axis_size("row"), lax.axis_size("col")
    pairs, depth = pair_states.shape
    freqs, _, width = screening.shape
    held = pairs * (columns * depth * 2 + width * 2 + freqs * width * 4 + freqs * 512) + 3 * depth * width * 2
    fits = depth % 128 == 0 and width == rows * depth and columns % CORES == 0 and held < 60 * 2**20
    fits = fits and others[2].shape[0] == 128 and columns >= 2 * CORES
    return (fused if fits else shards)(pair_states, screening, *others)


def solution(mesh):
    in_specs = (P(None, ("row", "col")), P(None, "row", "col"), P(), P(), P(), P(), P())
    out_specs = (P(), P())
    return jax.shard_map(step, mesh=mesh, in_specs=in_specs, out_specs=out_specs, check_vma=False)
```
